128 devices in a mesh: block: 2 (over z_lo), span: 8 (over y, x_lo), group: 8 (over z_hi, x_hi, core).
Axes of the slice: x: 4 (x_hi: 2, x_lo: 2; x = x_hi * 2 + x_lo), y: 4, z: 4 (z_hi: 2, z_lo: 2; z = z_hi * 2 + z_lo), core: 2. Of those that a mesh axis runs over, the one named last changes fastest.
Arguments:
- key_rows: bfloat16 [16, 24576, 8, 128], P(None, ('block', 'span'), 'group'), may hold values from -6 to 6
- value_rows: bfloat16 [16, 24576, 8, 128], P(None, ('block', 'span'), 'group'), may hold values from -6 to 6
- turn_angle: float32 [24576, 64], replicated, may hold values from -3.140625 to 3.140625
- key_gain: float32 [128], replicated, may hold values from 0.25 to 1.75
Outputs:
- stored_keys: bfloat16 [16, 8, 128, 24576], P(('block', 'span'), 'group')
- stored_values: bfloat16 [16, 24576, 8, 128], P(('block', 'span'), None, 'group')
- key_scale: float32 [16, 8, 128], P(('block', 'span'), 'group')
The draws below stay inside these ranges and needn't reach their ends.
All inputs are finite; a program needn't handle non-finite values. Where the reference program divides by a largest or mean magnitude, that divisor is 1e-20 or more.
Results may differ from the reference program's by a relative error of at most 0.001.
Values may be sent and summed in bfloat16 or wider, within the bound.
A program may use at most 128 MiB of HBM per device.

```python
import jax
import jax.numpy as jnp
from jax import lax

BATCH = 16
LENGTH = 24576
KV_HEADS = 8
HEAD_SIZE = 128
HALF_HEAD = 64


def shard_levels(key, dims, pieces, smallest, largest):
    factor_of = 1.0
    for axis_at, parts in pieces:
        heights = jax.random.uniform(jax.random.fold_in(jax.random.fold_in(key, 6), axis_at), (parts,), jnp.float32, smallest / len(pieces), largest / len(pieces))
        factor_of = factor_of * jnp.repeat(jnp.exp(heights), dims[axis_at] // parts).reshape((-1,) + (1,) * (len(dims) - 1 - axis_at))
    return factor_of


def gaussian(rng, extent, spread, reach, split=(), dtype=jnp.bfloat16):
    factor_of = shard_levels(rng, extent, split, -0.22, 0.18) if split else 1.0
    array = jax.random.normal(rng, extent, jnp.float32) * spread * factor_of
    return jnp.minimum(jnp.maximum(array, -reach), reach).astype(dtype)


def setup_inputs(seed: int = 0) -> dict:
    key_list = jax.random.split(jax.random.key(seed), 5)
    key_rows = gaussian(key_list[0], (BATCH, LENGTH, KV_HEADS, HEAD_SIZE), 1.0, 6.0, ((1, 16), (2, 8)))
    value_rows = gaussian(key_list[1], (BATCH, LENGTH, KV_HEADS, HEAD_SIZE), 1.0, 6.0, ((1, 16), (2, 8)))
    turn_angle = jnp.clip(jax.random.uniform(key_list[2], (LENGTH, HALF_HEAD), jnp.float32, -3.140625, 3.140625), -3.140625, 3.140625)
    key_gain = jnp.clip(1.0 + 0.15 * jax.random.normal(key_list[3], (HEAD_SIZE,), jnp.float32), 0.25, 1.75)
    return dict(key_rows=key_rows, value_rows=value_rows, turn_angle=turn_angle, key_gain=key_gain)


def apply_rotary(vectors, angle):
    half = vectors.shape[-1] // 2
    cosine, sine = (jnp.cos(angle)[None, :, None, :], jnp.sin(angle)[None, :, None, :])
    first, second = (vectors[..., :half], vectors[..., half:])
    return jnp.concatenate([first * cosine - second * sine, second * cosine + first * sine], axis=-1)

def unit_rows(vectors, row_gain):
    return vectors * lax.rsqrt(lax.optimization_barrier(jnp.mean(vectors * vectors, axis=-1, keepdims=True)) + 1e-06) * row_gain

def ready_to_store(plain_keys, angle, key_gain):
    wide_keys = plain_keys.astype(jnp.float32)
    wide_keys = unit_rows(wide_keys, key_gain)
    return apply_rotary(wide_keys, angle)

def reference(key_rows, value_rows, turn_angle, key_gain):
    turned_keys = ready_to_store(key_rows, turn_angle, key_gain)
    key_scale = lax.optimization_barrier(jnp.max(jnp.abs(turned_keys), axis=1))
    narrow_keys = (turned_keys / key_scale[:, None]).astype(jnp.bfloat16)
    stored_keys = jnp.transpose(narrow_keys, (0, 2, 3, 1))
    stored_values = value_rows
    return (stored_keys, stored_values, key_scale)
```

```python
import functools

import jax
import jax.numpy as jnp
from jax import lax
from jax.experimental import pallas as pl
from jax.experimental.pallas import tpu as pltpu
from jax.sharding import PartitionSpec as P

MESH = pl.DeviceIdType.MESH
ORDER = ("xzy", "zyx", "yxz")
STEP = {"x": (1, 0, 0), "z": (0, 0, 1), "p": (0, 1, 0), "m": (0, 3, 0)}
OFFSETS = [(x, y, z) for x in range(2) for y in range(4) for z in range(2) if x or y or z]
TILE = 128


def path(offset, order):
    dx, dy, dz = offset
    links = {
        "x": ["x"] * dx,
        "z": ["z"] * dz,
        "y": [[], ["p"], ["p", "p"] if (dx + dz) % 2 == 0 else ["m", "m"], ["m"]][dy],
    }
    return [link for axis in order for link in links[axis]]


def plan():
    hops = []
    for array in range(2):
        for strip, order in enumerate(ORDER):
            for phase, axis in enumerate(order):
                for link in "pm" if axis == "y" else axis:
                    items = []
                    for offset in OFFSETS:
                        links = path(offset, order)
                        for at, name in enumerate(links):
                            if name == link:
                                again = at > 0 and links[at - 1] == link
                                first = link in "pm" and offset[1] == 2 and not again
                                left = len(links) - at - 1
                                key = (4 * again - first, at > again, -left)
                                items.append((key, offset, at, left == 0))
                    for i, (_, offset, at, last) in enumerate(sorted(items)):
                        hops.append(
                            dict(
                                array=array,
                                strip=strip,
                                offset=offset,
                                at=at,
                                link=link,
                                last=last,
                                time=(array * 3 + phase) * 8 + i,
                                done=path(offset, order)[:at],
                            )
                        )
    hops.sort(key=lambda h: (h["time"], "xzpm".index(h["link"])))
    where = {(h["array"], h["strip"], h["offset"], h["at"]): i for i, h in enumerate(hops)}
    slots = 0
    for h in hops:
        h["after"] = where[h["array"], h["strip"], h["offset"], h["at"] - 1] if h["at"] else None
        h["slot"] = None
        if not h["last"]:
            h["slot"], slots = slots, slots + 1
    return hops, slots


def kernel(
    hops, angle, gain, keys, values, out_keys, out_values, out_scale,
    raw, table, transit, gains, top, send, recv, local,
):
    blocks, rows, size = raw.shape
    half = size // 2
    length = blocks * rows
    strip_rows = rows // len(ORDER)
    z = lax.axis_index("block")
    y = lax.axis_index("span") // 2
    x = lax.axis_index("span") % 2

    def device(step):
        return {"block": (z + step[2]) % 2, "span": ((y + step[1]) % 4) * 2 + (x + step[0]) % 2}

    def block_at(dx, dy, dz):
        return ((z + dz) % 2) * 8 + ((y + dy) % 4) * 2 + (x + dx) % 2

    barrier = pltpu.get_barrier_semaphore()
    for step in STEP.values():
        pl.semaphore_signal(barrier, inc=1, device_id=device(step), device_id_type=MESH)
    pl.semaphore_wait(barrier, len(STEP))

    copies = [None] * len(hops)
    received = set()

    def arrived(i):
        if i not in received:
            copies[i].wait_recv()
            received.add(i)

    def start(i):
        hop = hops[i]
        span = pl.ds(hop["strip"] * strip_rows, strip_rows)
        if hop["after"] is None:
            source = (keys, values)[hop["array"]].at[block_at(*hop["offset"]), span]
        else:
            arrived(hop["after"])
            source = transit.at[hops[hop["after"]]["slot"]]
        if hop["last"]:
            gone = [sum(STEP[link][axis] for link in hop["done"]) for axis in range(3)]
            target = (raw, out_values)[hop["array"]].at[
                block_at(gone[0], 8 - gone[1], gone[2]), span
            ]
        else:
            target = transit.at[hop["slot"]]
        copies[i] = pltpu.make_async_remote_copy(
            src_ref=source,
            dst_ref=target,
            send_sem=send.at[i],
            recv_sem=recv.at[i],
            device_id=device(STEP[hop["link"]]),
            device_id_type=MESH,
        )
        copies[i].start()

    me = block_at(0, 0, 0)
    angles_in = pltpu.make_async_copy(angle, table.at[pl.ds(0, half)], local.at[0])
    keys_in = pltpu.make_async_copy(keys.at[me], raw.at[me], local.at[1])
    values_in = pltpu.make_async_copy(values.at[me], out_values.at[me], local.at[2])

    def columns(i, width):
        return pl.ds(pl.multiple_of(i * width, width), width)

    def turns(begin, end):
        def body(i, _):
            a = table[:half, columns(i, TILE)]
            table[:half, columns(i, TILE)] = jnp.cos(a)
            table[half:, columns(i, TILE)] = jnp.sin(a)
            return 0

        lax.fori_loop(begin // TILE, end // TILE, body, 0)

    def turn(begin, end):
        def body(i, high):
            block, row = i // (rows // TILE), i % (rows // TILE)
            wide = raw[block, columns(row, TILE), :].astype(jnp.float32).T
            mean = jnp.sum(wide * wide, axis=0, keepdims=True) / size
            wide = wide * lax.rsqrt(mean + 1e-06) * gains[...]
            cosine, sine = table[:half, columns(i, TILE)], table[half:, columns(i, TILE)]
            first, second = wide[:half], wide[half:]
            one = first * cosine - second * sine
            two = second * cosine + first * sine
            table[:half, columns(i, TILE)] = one
            table[half:, columns(i, TILE)] = two
            return jnp.maximum(high, jnp.abs(jnp.concatenate([one, two], axis=0)))

        top[...] = lax.fori_loop(begin // TILE, end // TILE, body, top[...])

    def scale_up():
        high = jnp.broadcast_to(jnp.max(top[...], axis=1, keepdims=True), (size, TILE))
        top[...] = high
        out_scale[...] = high.T[:1]

    def narrow(begin, end):
        def body(i, _):
            out_keys[:, columns(i, TILE)] = (table[:, columns(i, TILE)] / top[...]).astype(jnp.bfloat16)
            return 0

        lax.fori_loop(begin // TILE, end // TILE, body, 0)

    times = hops[-1]["time"] + 1
    at_time = [[i for i, h in enumerate(hops) if h["time"] == t] for t in range(times)]
    third = times // 2
    for t in range(times):
        for i in at_time[t]:
            start(i)
        if t == 0:
            angles_in.start()
            keys_in.start()
            values_in.start()
            gains[...] = jnp.broadcast_to(gain[...], (TILE, size)).T
            top[...] = jnp.zeros_like(top)
            angles_in.wait()
        if t < third:
            turns(t * length // third, (t + 1) * length // third)
        elif t == third + 2:
            keys_in.wait()
            for i, h in enumerate(hops):
                if h["array"] == 0 and h["last"]:
                    arrived(i)
        elif third + 2 < t <= third + 10:
            turn((t - third - 3) * length // 8, (t - third - 2) * length // 8)
        elif t == third + 11:
            scale_up()
        elif third + 11 < t <= third + 19:
            narrow((t - third - 12) * length // 8, (t - third - 11) * length // 8)
    values_in.wait()
    for i in range(len(hops)):
        arrived(i)
    for copy in copies:
        copy.wait_send()


def body(key_rows, value_rows, turn_angle, key_gain):
    blocks, rows, heads, size = key_rows.shape
    length = blocks * rows
    hops, slots = plan()
    strip_rows = rows // len(ORDER)
    vmem, hbm = pl.BlockSpec(memory_space=pltpu.VMEM), pl.BlockSpec(memory_space=pl.ANY)
    stored_keys, stored_values, key_scale = pl.pallas_call(
        functools.partial(kernel, hops),
        name="hand_over",
        out_shape=(
            pltpu.VMEM((size, length), jnp.bfloat16),
            pltpu.VMEM((blocks, rows, size), jnp.bfloat16),
            jax.ShapeDtypeStruct((1, size), jnp.float32),
        ),
        in_specs=[hbm, vmem, hbm, hbm],
        out_specs=(vmem, vmem, vmem),
        scratch_shapes=[
            pltpu.VMEM((blocks, rows, size), jnp.bfloat16),
            pltpu.VMEM((size, length), jnp.float32),
            pltpu.VMEM((slots, strip_rows, size), jnp.bfloat16),
            pltpu.VMEM((size, TILE), jnp.float32),
            pltpu.VMEM((size, TILE), jnp.float32),
            pltpu.SemaphoreType.DMA((len(hops),)),
            pltpu.SemaphoreType.DMA((len(hops),)),
            pltpu.SemaphoreType.DMA((3,)),
        ],
        compiler_params=pltpu.CompilerParams(
            collective_id=0, has_side_effects=True, vmem_limit_bytes=36 << 20
        ),
    )(
        turn_angle.T,
        key_gain.reshape(1, size),
        key_rows.reshape(blocks, rows, size),
        value_rows.reshape(blocks, rows, size),
    )
    return (
        stored_keys.reshape(1, 1, size, length),
        stored_values.reshape(1, length, 1, size),
        key_scale.reshape(1, 1, size),
    )


def solution(mesh):
    return jax.shard_map(
        body,
        mesh=mesh,
        in_specs=(
            P(None, ("block", "span"), "group", None),
            P(None, ("block", "span"), "group", None),
            P(),
            P(),
        ),
        out_specs=(
            P(("block", "span"), "group", None, None),
            P(("block", "span"), None, "group", None),
            P(("block", "span"), "group", None),
        ),
        check_vma=False,
    )
```

```python
import functools

import jax
import jax.numpy as jnp
from jax import lax
from jax.experimental import pallas as pl
from jax.experimental.pallas import tpu as pltpu
from jax.sharding import PartitionSpec as P

MESH = pl.DeviceIdType.MESH
STEP = {"x": (1, 0, 0), "z": (0, 0, 1), "p": (0, 1, 0), "m": (0, 3, 0)}
ROUTES = (
    (0, (0, 2, 0), "mm", (2, 8)),
    (0, (1, 1, 0), "px", (2, 8)),
    (0, (0, 1, 0), "p", (9,)),
    (0, (0, 2, 1), "ppz", (0, 4, 9)),
    (0, (1, 0, 1), "zx", (3, 9)),
    (0, (1, 2, 0), "xmm", (0, 4, 9)),
    (0, (0, 3, 1), "zm", (4, 10)),
    (0, (1, 0, 0), "x", (10,)),
    (0, (1, 2, 1), "zxpp", (0, 3, 6, 10)),
    (0, (1, 3, 1), "mxz", (1, 5, 10)),
    (0, (0, 1, 1), "pz", (3, 11)),
    (0, (0, 3, 0), "m", (11,)),
    (0, (1, 1, 1), "zpx", (1, 5, 11)),
    (0, (0, 0, 1), "z", (12,)),
    (0, (1, 3, 0), "mx", (3, 12)),
    (1, (0, 2, 1), "pzp", (1, 7, 11)),
    (1, (0, 1, 0), "p", (12,)),
    (1, (0, 3, 1), "zm", (5, 12)),
    (1, (0, 3, 0), "m", (13,)),
    (1, (1, 0, 1), "xz", (7, 13)),
    (1, (1, 1, 0), "xp", (6, 13)),
    (1, (1, 3, 0), "mx", (7, 13)),
    (1, (0, 1, 1), "pz", (7, 14)),
    (1, (0, 2, 0), "mm", (5, 14)),
    (1, (1, 1, 1), "xzp", (1, 6, 14)),
    (1, (1, 3, 1), "zmx", (2, 6, 14)),
    (1, (0, 0, 1), "z", (15,)),
    (1, (1, 0, 0), "x", (15,)),
    (1, (1, 2, 0), "xpp", (2, 8, 15)),
    (1, (1, 2, 1), "mxzm", (0, 4, 8, 15)),
)
STEPS = 16
AHEAD = 2
TURNS_STEPS = 8
TILE = 128


def plan():
    hops, slots = [], 0
    for array, offset, links, times in ROUTES:
        for at, (link, time) in enumerate(zip(links, times)):
            last = at + 1 == len(links)
            hops.append(
                dict(
                    array=array, offset=offset, at=at, link=link, time=time, done=links[:at],
                    slot=None if last else slots,
                )
            )
            slots += not last
    hops.sort(key=lambda hop: hop["time"])
    where = {(hop["array"], hop["offset"], hop["at"]): i for i, hop in enumerate(hops)}
    for hop in hops:
        hop["after"] = where.get((hop["array"], hop["offset"], hop["at"] - 1))
    return hops, slots


def kernel(
    hops, angle, gain, keys, values, out_keys, out_values, out_scale,
    raw, table, transit, gain_row, gains, top, send, recv, local,
):
    blocks, rows, size = raw.shape
    half = size // 2
    length = blocks * rows
    z = lax.axis_index("block")
    y = lax.axis_index("span") // 2
    x = lax.axis_index("span") % 2

    def device(step):
        return {"block": (z + step[2]) % 2, "span": ((y + step[1]) % 4) * 2 + (x + step[0]) % 2}

    def block_at(dx, dy, dz):
        return ((z + dz) % 2) * 8 + ((y + dy) % 4) * 2 + (x + dx) % 2

    me = block_at(0, 0, 0)
    gain_in = pltpu.make_async_copy(gain, gain_row, local.at[0])
    angles_in = pltpu.make_async_copy(angle, table.at[pl.ds(0, half)], local.at[1])
    keys_in = pltpu.make_async_copy(keys.at[me], raw.at[me], local.at[2])
    values_in = pltpu.make_async_copy(values.at[me], out_values.at[me], local.at[3])

    barrier = pltpu.get_barrier_semaphore()
    for step in STEP.values():
        pl.semaphore_signal(barrier, inc=1, device_id=device(step), device_id_type=MESH)
    pl.semaphore_wait(barrier, len(STEP))

    copies = [None] * len(hops)
    received = set()

    def arrived(i):
        if i not in received:
            copies[i].wait_recv()
            received.add(i)

    def start(i):
        hop = hops[i]
        if hop["after"] is None:
            source = (keys, values)[hop["array"]].at[block_at(*hop["offset"])]
        else:
            arrived(hop["after"])
            source = transit.at[hops[hop["after"]]["slot"]]
        if hop["slot"] is None:
            gone = [sum(STEP[link][axis] for link in hop["done"]) for axis in range(3)]
            target = (raw, out_values)[hop["array"]].at[block_at(gone[0], 8 - gone[1], gone[2])]
        else:
            target = transit.at[hop["slot"]]
        copies[i] = pltpu.make_async_remote_copy(
            src_ref=source,
            dst_ref=target,
            send_sem=send.at[i],
            recv_sem=recv.at[i],
            device_id=device(STEP[hop["link"]]),
            device_id_type=MESH,
        )
        copies[i].start()

    def columns(i):
        return pl.ds(pl.multiple_of(i * TILE, TILE), TILE)

    def turns(begin, end):
        def body(i, _):
            a = table[:half, columns(i)]
            table[:half, columns(i)] = jnp.cos(a)
            table[half:, columns(i)] = jnp.sin(a)
            return 0

        lax.fori_loop(begin, end, body, 0)

    def turn(block):
        def body(i, high):
            at = columns(block * (rows // TILE) + i)
            wide = raw[block, columns(i), :].astype(jnp.float32).T
            mean = jnp.sum(wide * wide, axis=0, keepdims=True) / size
            wide = wide * lax.rsqrt(mean + 1e-06) * gains[...]
            cosine, sine = table[:half, at], table[half:, at]
            first, second = wide[:half], wide[half:]
            one = first * cosine - second * sine
            two = second * cosine + first * sine
            table[:half, at] = one
            table[half:, at] = two
            return jnp.maximum(high, jnp.abs(jnp.concatenate([one, two], axis=0)))

        top[...] = lax.fori_loop(0, rows // TILE, body, top[...])

    def narrow():
        high = jnp.broadcast_to(jnp.max(top[...], axis=1, keepdims=True), (size, TILE))
        top[...] = high
        out_scale[...] = high.T[:1]

        def body(i, _):
            out_keys[:, columns(i)] = (table[:, columns(i)] / top[...]).astype(jnp.bfloat16)
            return 0

        lax.fori_loop(0, length // TILE, body, 0)

    def start_step(time):
        for i, hop in enumerate(hops):
            if hop["time"] == time:
                start(i)

    for time in range(AHEAD):
        start_step(time)
    for copy in (gain_in, angles_in, keys_in, values_in):
        copy.start()
    gain_in.wait()
    gains[...] = jnp.broadcast_to(gain_row[...], (TILE, size)).T
    top[...] = jnp.zeros_like(top)
    angles_in.wait()
    keys_in.wait()
    tiles = length // TILE
    final = [(hop["time"], i) for i, hop in enumerate(hops) if hop["array"] == 0 and hop["slot"] is None]
    for time in range(STEPS):
        start_step(time + AHEAD)
        if time < TURNS_STEPS:
            turns(time * tiles // TURNS_STEPS, (time + 1) * tiles // TURNS_STEPS)
        if time == TURNS_STEPS:
            turn(me)
        for came, i in final:
            if max(came + 1, TURNS_STEPS) == time:
                arrived(i)
                dx, dy, dz = hops[i]["offset"]
                turn(block_at(dx, 4 - dy, dz))
        if time == max(final)[0] + 1:
            narrow()
    values_in.wait()
    for i in range(len(hops)):
        arrived(i)
    for copy in copies:
        copy.wait_send()


def store(keys, values, scale, out_keys, out_values, out_scale, done):
    parts = done.shape[0] // 2
    copies = [pltpu.make_async_copy(scale, out_scale, done.at[2 * parts])]
    for j, (source, target) in enumerate(((keys, out_keys), (values, out_values))):
        step = source.shape[0] // parts
        for i in range(parts):
            part = pl.ds(i * step, step)
            copies.append(
                pltpu.make_async_copy(source.at[part], target.at[part], done.at[j * parts + i])
            )
    for copy in copies:
        copy.start()
    for copy in copies:
        copy.wait()


def body(key_rows, value_rows, turn_angle, key_gain):
    blocks, rows, heads, size = key_rows.shape
    length = blocks * rows
    hops, slots = plan()
    vmem, hbm = pl.BlockSpec(memory_space=pltpu.VMEM), pl.BlockSpec(memory_space=pl.ANY)
    outputs = (
        ((size, length), jnp.bfloat16),
        ((blocks, rows, size), jnp.bfloat16),
        ((1, size), jnp.float32),
    )
    held = pl.pallas_call(
        functools.partial(kernel, hops),
        name="hand_over",
        out_shape=tuple(pltpu.VMEM(*output) for output in outputs),
        in_specs=[hbm, pl.BlockSpec(memory_space=pltpu.HBM), hbm, hbm],
        out_specs=(vmem,) * 3,
        scratch_shapes=[
            pltpu.VMEM((blocks, rows, size), jnp.bfloat16),
            pltpu.VMEM((size, length), jnp.float32),
            pltpu.VMEM((slots, rows, size), jnp.bfloat16),
            pltpu.VMEM((1, size), jnp.float32),
            pltpu.VMEM((size, TILE), jnp.float32),
            pltpu.VMEM((size, TILE), jnp.float32),
            pltpu.SemaphoreType.DMA((len(hops),)),
            pltpu.SemaphoreType.DMA((len(hops),)),
            pltpu.SemaphoreType.DMA((4,)),
        ],
        compiler_params=pltpu.CompilerParams(
            collective_id=0, has_side_effects=True, vmem_limit_bytes=36 << 20
        ),
    )(
        turn_angle.T,
        key_gain.reshape(1, size),
        key_rows.reshape(blocks, rows, size),
        value_rows.reshape(blocks, rows, size),
    )
    stored_keys, stored_values, key_scale = pl.pallas_call(
        store,
        name="store",
        out_shape=tuple(jax.ShapeDtypeStruct(*output) for output in outputs),
        in_specs=[hbm] * 3,
        out_specs=(hbm,) * 3,
        scratch_shapes=[pltpu.SemaphoreType.DMA((9,))],
        compiler_params=pltpu.CompilerParams(vmem_limit_bytes=2 << 20),
    )(*held)
    return (
        stored_keys.reshape(1, 1, size, length),
        stored_values.reshape(1, length, 1, size),
        key_scale.reshape(1, 1, size),
    )


def solution(mesh):
    return jax.shard_map(
        body,
        mesh=mesh,
        in_specs=(
            P(None, ("block", "span"), "group", None),
            P(None, ("block", "span"), "group", None),
            P(),
            P(),
        ),
        out_specs=(
            P(("block", "span"), "group", None, None),
            P(("block", "span"), None, "group", None),
            P(("block", "span"), "group", None),
        ),
        check_vma=False,
    )
```

```python
import functools

import jax
import jax.numpy as jnp
from jax import lax
from jax.experimental import pallas as pl
from jax.experimental.pallas import tpu as pltpu
from jax.sharding import PartitionSpec as P

MESH = pl.DeviceIdType.MESH
STEP = {"x": (1, 0, 0), "z": (0, 0, 1), "p": (0, 1, 0), "m": (0, 3, 0)}
ROUTES = (
    (0, (0, 2, 0), "mm", (2, 8)),
    (0, (1, 1, 0), "px", (2, 8)),
    (0, (0, 1, 0), "p", (9,)),
    (0, (0, 2, 1), "ppz", (0, 4, 9)),
    (0, (1, 0, 1), "zx", (3, 9)),
    (0, (1, 2, 0), "xmm", (0, 4, 9)),
    (0, (0, 3, 1), "zm", (4, 10)),
    (0, (1, 0, 0), "x", (10,)),
    (0, (1, 2, 1), "zxpp", (0, 3, 6, 10)),
    (0, (1, 3, 1), "mxz", (1, 5, 10)),
    (0, (0, 1, 1), "pz", (3, 11)),
    (0, (0, 3, 0), "m", (11,)),
    (0, (1, 1, 1), "zpx", (1, 5, 11)),
    (0, (0, 0, 1), "z", (12,)),
    (0, (1, 3, 0), "mx", (3, 12)),
    (1, (0, 2, 1), "pzp", (1, 7, 11)),
    (1, (0, 1, 0), "p", (12,)),
    (1, (0, 3, 1), "zm", (5, 12)),
    (1, (0, 3, 0), "m", (13,)),
    (1, (1, 0, 1), "xz", (7, 13)),
    (1, (1, 1, 0), "xp", (6, 13)),
    (1, (1, 3, 0), "mx", (7, 13)),
    (1, (0, 1, 1), "pz", (7, 14)),
    (1, (0, 2, 0), "mm", (5, 14)),
    (1, (1, 1, 1), "xzp", (1, 6, 14)),
    (1, (1, 3, 1), "zmx", (2, 6, 14)),
    (1, (0, 0, 1), "z", (15,)),
    (1, (1, 0, 0), "x", (15,)),
    (1, (1, 2, 0), "xpp", (2, 8, 15)),
    (1, (1, 2, 1), "mxzm", (0, 4, 8, 15)),
)
STEPS = 16
AHEAD = 2
SPLIT = 14
TURNS_STEPS = 8
TILE = 128
KEY_PARTS = 4


def plan():
    hops, slots = [], 0
    for array, offset, links, times in ROUTES:
        for at, (link, time) in enumerate(zip(links, times)):
            last = at + 1 == len(links)
            hops.append(
                dict(
                    array=array, offset=offset, at=at, link=link, time=time, done=links[:at],
                    slot=None if last else slots,
                )
            )
            slots += not last
    hops.sort(key=lambda hop: hop["time"])
    where = {(hop["array"], hop["offset"], hop["at"]): i for i, hop in enumerate(hops)}
    for hop in hops:
        hop["after"] = where.get((hop["array"], hop["offset"], hop["at"] - 1))
    return hops, slots


def late_hops(hops):
    return [i for i, hop in enumerate(hops) if hop["time"] >= SPLIT]


def core():
    return lax.axis_index("group") % 2


def device(step):
    z, y, x = lax.axis_index("block"), lax.axis_index("span") // 2, lax.axis_index("span") % 2
    return {"block": (z + step[2]) % 2, "span": ((y + step[1]) % 4) * 2 + (x + step[0]) % 2}


def block_at(dx, dy, dz):
    z, y, x = lax.axis_index("block"), lax.axis_index("span") // 2, lax.axis_index("span") % 2
    return ((z + dz) % 2) * 8 + ((y + dy) % 4) * 2 + (x + dx) % 2


def came_from(offset):
    return block_at(offset[0], 4 - offset[1], offset[2])


def meet():
    barrier = pltpu.get_barrier_semaphore()
    for step in STEP.values():
        pl.semaphore_signal(barrier, inc=1, device_id=device(step), device_id_type=MESH)
    pl.semaphore_wait(barrier, len(STEP))


def kernel(
    hops, angle, gain, keys, values, out_keys, out_values, out_scale, transit,
    raw, table, gain_row, gains, top, send, recv, local,
):
    blocks, rows, size = raw.shape
    half = size // 2
    length = blocks * rows

    me = block_at(0, 0, 0)
    gain_in = pltpu.make_async_copy(gain, gain_row, local.at[0])
    angles_in = pltpu.make_async_copy(angle, table.at[pl.ds(0, half)], local.at[1])
    keys_in = pltpu.make_async_copy(keys.at[me], raw.at[me], local.at[2])
    values_in = pltpu.make_async_copy(values.at[me], out_values.at[me], local.at[3])

    meet()
    copies = [None] * len(hops)
    received = set()

    def arrived(i):
        if i not in received:
            copies[i].wait_recv()
            received.add(i)

    def start(i):
        hop = hops[i]
        if hop["after"] is None:
            source = (keys, values)[hop["array"]].at[block_at(*hop["offset"])]
        else:
            arrived(hop["after"])
            source = transit.at[hops[hop["after"]]["slot"]]
        if hop["slot"] is None:
            gone = [sum(STEP[link][axis] for link in hop["done"]) for axis in range(3)]
            target = (raw, out_values)[hop["array"]].at[block_at(gone[0], 8 - gone[1], gone[2])]
        else:
            target = transit.at[hop["slot"]]
        copies[i] = pltpu.make_async_remote_copy(
            src_ref=source,
            dst_ref=target,
            send_sem=send.at[i],
            recv_sem=recv.at[i],
            device_id=device(STEP[hop["link"]]),
            device_id_type=MESH,
        )
        if hop["time"] < SPLIT:
            copies[i].start()
        else:
            pl.when(core() == 1)(copies[i].start)

    def columns(i):
        return pl.ds(pl.multiple_of(i * TILE, TILE), TILE)

    def turns(begin, end):
        def body(i, _):
            a = table[:half, columns(i)]
            table[:half, columns(i)] = jnp.cos(a)
            table[half:, columns(i)] = jnp.sin(a)
            return 0

        lax.fori_loop(begin, end, body, 0)

    def turn(block):
        def body(i, high):
            at = columns(block * (rows // TILE) + i)
            wide = raw[block, columns(i), :].astype(jnp.float32).T
            mean = jnp.sum(wide * wide, axis=0, keepdims=True) / size
            wide = wide * lax.rsqrt(mean + 1e-06) * gains[...]
            cosine, sine = table[:half, at], table[half:, at]
            first, second = wide[:half], wide[half:]
            one = first * cosine - second * sine
            two = second * cosine + first * sine
            table[:half, at] = one
            table[half:, at] = two
            return jnp.maximum(high, jnp.abs(jnp.concatenate([one, two], axis=0)))

        top[...] = lax.fori_loop(0, rows // TILE, body, top[...])

    def narrow():
        high = jnp.broadcast_to(jnp.max(top[...], axis=1, keepdims=True), (size, TILE))
        top[...] = high
        out_scale[...] = high.T[:1]

        def body(i, _):
            out_keys[:, columns(i)] = (table[:, columns(i)] / top[...]).astype(jnp.bfloat16)
            return 0

        lax.fori_loop(0, length // TILE, body, 0)

    def start_step(time):
        for i, hop in enumerate(hops):
            if hop["time"] == time:
                start(i)

    for copy in (gain_in, angles_in, keys_in, values_in):
        copy.start()
    pl.when(core() == 1)(angles_in.wait)
    for time in range(AHEAD):
        start_step(time)
    pl.when(core() == 0)(angles_in.wait)
    gain_in.wait()
    gains[...] = jnp.broadcast_to(gain_row[...], (TILE, size)).T
    top[...] = jnp.zeros_like(top)
    keys_in.wait()
    tiles = length // TILE
    final = [(hop["time"], i) for i, hop in enumerate(hops) if hop["array"] == 0 and hop["slot"] is None]
    for time in range(STEPS):
        start_step(time + AHEAD)
        if time < TURNS_STEPS:
            turns(time * tiles // TURNS_STEPS, (time + 1) * tiles // TURNS_STEPS)
        if time == TURNS_STEPS:
            turn(me)
        for came, i in final:
            if max(came + 1, TURNS_STEPS) == time:
                arrived(i)
                turn(came_from(hops[i]["offset"]))
        if time == max(final)[0] + 1:
            narrow()
    values_in.wait()
    for i, hop in enumerate(hops):
        if hop["time"] < SPLIT:
            arrived(i)
            copies[i].wait_send()

    @pl.when(core() == 1)
    def _():
        for i in late_hops(hops):
            copies[i].wait()


def late(hops, values, transit, _, landed, send, recv):
    meet()

    @pl.when(core() == 0)
    def _():
        copies = []
        for j, i in enumerate(late_hops(hops)):
            hop = hops[i]
            if hop["after"] is None:
                source = values.at[block_at(*hop["offset"])]
            else:
                source = transit.at[hops[hop["after"]]["slot"]]
            copy = pltpu.make_async_remote_copy(
                src_ref=source,
                dst_ref=landed.at[j],
                send_sem=send.at[j],
                recv_sem=recv.at[j],
                device_id=device(STEP[hop["link"]]),
                device_id_type=MESH,
            )
            copy.start()
            copies.append(copy)
        for copy in copies:
            copy.wait()


def store(hops, keys, values, scale, out_keys, out_values, out_scale, done):
    blocks = values.shape[0]
    part = keys.shape[0] // KEY_PARTS
    copies = [pltpu.make_async_copy(scale, out_scale, done.at[0])]
    for i in range(KEY_PARTS):
        at = pl.ds(i * part, part)
        copies.append(pltpu.make_async_copy(keys.at[at], out_keys.at[at], done.at[1 + i]))
    offsets = [hops[i]["offset"] for i in late_hops(hops)]
    offsets += [(0, 0, 0)] + [
        hop["offset"] for hop in hops if hop["array"] == 1 and hop["slot"] is None and hop["time"] < SPLIT
    ]
    moves = []
    for i, offset in enumerate(offsets):
        at = came_from(offset)
        moves.append(
            pltpu.make_async_copy(values.at[at], out_values.at[at], done.at[1 + KEY_PARTS + i])
        )
    assert len(moves) == blocks
    later = len(late_hops(hops))
    for copy in copies + moves[later:]:
        copy.start()

    @pl.when(core() == 1)
    def _():
        for copy in moves[:later]:
            copy.start()
        for copy in moves[:later]:
            copy.wait()

    for copy in copies + moves[later:]:
        copy.wait()


def store_late(hops, landed, stored, out_values, done):
    @pl.when(core() == 0)
    def _():
        copies = []
        for j, i in enumerate(late_hops(hops)):
            target = out_values.at[came_from(hops[i]["offset"])]
            copies.append(pltpu.make_async_copy(landed.at[j], target, done.at[j]))
        for copy in copies:
            copy.start()
        for copy in copies:
            copy.wait()


def body(key_rows, value_rows, turn_angle, key_gain):
    blocks, rows, heads, size = key_rows.shape
    length = blocks * rows
    hops, slots = plan()
    turn_angle, key_gain, key_rows, value_rows = (
        pltpu.with_memory_space_constraint(array, pltpu.HBM)
        for array in (
            turn_angle.T,
            key_gain.reshape(1, size),
            key_rows.reshape(blocks, rows, size),
            value_rows.reshape(blocks, rows, size),
        )
    )
    vmem, hbm = pl.BlockSpec(memory_space=pltpu.VMEM), pl.BlockSpec(memory_space=pl.ANY)
    outputs = (
        ((size, length), jnp.bfloat16),
        ((blocks, rows, size), jnp.bfloat16),
        ((1, size), jnp.float32),
    )
    later = len(late_hops(hops))
    *held, transit = pl.pallas_call(
        functools.partial(kernel, hops),
        name="hand_over",
        out_shape=tuple(pltpu.VMEM(*output) for output in outputs)
        + (pltpu.VMEM((slots, rows, size), jnp.bfloat16),),
        in_specs=[hbm] * 4,
        out_specs=(vmem,) * 4,
        scratch_shapes=[
            pltpu.VMEM((blocks, rows, size), jnp.bfloat16),
            pltpu.VMEM((size, length), jnp.float32),
            pltpu.VMEM((1, size), jnp.float32),
            pltpu.VMEM((size, TILE), jnp.float32),
            pltpu.VMEM((size, TILE), jnp.float32),
            pltpu.SemaphoreType.DMA((len(hops),)),
            pltpu.SemaphoreType.DMA((len(hops),)),
            pltpu.SemaphoreType.DMA((4,)),
        ],
        compiler_params=pltpu.CompilerParams(
            collective_id=0, has_side_effects=True, vmem_limit_bytes=22 << 20
        ),
    )(turn_angle, key_gain, key_rows, value_rows)
    stored_keys, stored_values, key_scale = pl.pallas_call(
        functools.partial(store, hops),
        name="store",
        out_shape=tuple(jax.ShapeDtypeStruct(*output) for output in outputs),
        in_specs=[hbm] * 3,
        out_specs=(hbm,) * 3,
        scratch_shapes=[pltpu.SemaphoreType.DMA((1 + KEY_PARTS + blocks,))],
        compiler_params=pltpu.CompilerParams(vmem_limit_bytes=1 << 20),
    )(*held)
    landed = pl.pallas_call(
        functools.partial(late, hops),
        name="late",
        out_shape=pltpu.VMEM((later, rows, size), jnp.bfloat16),
        in_specs=[hbm] * 3,
        out_specs=vmem,
        scratch_shapes=[pltpu.SemaphoreType.DMA((later,)), pltpu.SemaphoreType.DMA((later,))],
        compiler_params=pltpu.CompilerParams(
            collective_id=1, has_side_effects=True, vmem_limit_bytes=1 << 20
        ),
    )(value_rows, transit, pltpu.with_memory_space_constraint(key_scale, pltpu.HBM))
    stored_values = pl.pallas_call(
        functools.partial(store_late, hops),
        name="store_late",
        out_shape=jax.ShapeDtypeStruct(*outputs[1]),
        in_specs=[hbm] * 2,
        out_specs=hbm,
        scratch_shapes=[pltpu.SemaphoreType.DMA((later,))],
        input_output_aliases={1: 0},
        compiler_params=pltpu.CompilerParams(vmem_limit_bytes=1 << 20),
    )(landed, stored_values)
    return (
        stored_keys.reshape(1, 1, size, length),
        stored_values.reshape(1, length, 1, size),
        key_scale.reshape(1, 1, size),
    )


def solution(mesh):
    return jax.shard_map(
        body,
        mesh=mesh,
        in_specs=(
            P(None, ("block", "span"), "group", None),
            P(None, ("block", "span"), "group", None),
            P(),
            P(),
        ),
        out_specs=(
            P(("block", "span"), "group", None, None),
            P(("block", "span"), None, "group", None),
            P(("block", "span"), "group", None),
        ),
        check_vma=False,
    )
```

```python
import functools

import jax
import jax.numpy as jnp
from jax import lax
from jax.experimental import pallas as pl
from jax.experimental.pallas import tpu as pltpu
from jax.sharding import PartitionSpec as P

MESH = pl.DeviceIdType.MESH
STEP = {"x": (1, 0, 0), "z": (0, 0, 1), "p": (0, 1, 0), "m": (0, 3, 0)}
ROUTES = (
    (0, (0, 2, 0), "mm", (2, 8)),
    (0, (1, 1, 0), "px", (2, 8)),
    (0, (0, 1, 0), "p", (9,)),
    (0, (0, 2, 1), "ppz", (0, 4, 9)),
    (0, (1, 0, 1), "zx", (3, 9)),
    (0, (1, 2, 0), "xmm", (0, 4, 9)),
    (0, (0, 3, 1), "zm", (4, 10)),
    (0, (1, 0, 0), "x", (10,)),
    (0, (1, 2, 1), "zxpp", (0, 3, 6, 10)),
    (0, (1, 3, 1), "mxz", (1, 5, 10)),
    (0, (0, 1, 1), "pz", (3, 11)),
    (0, (0, 3, 0), "m", (11,)),
    (0, (1, 1, 1), "zpx", (1, 5, 11)),
    (0, (0, 0, 1), "z", (12,)),
    (0, (1, 3, 0), "mx", (3, 12)),
    (1, (0, 2, 1), "pzp", (1, 7, 11)),
    (1, (0, 1, 0), "p", (12,)),
    (1, (0, 3, 1), "zm", (5, 12)),
    (1, (0, 3, 0), "m", (13,)),
    (1, (1, 0, 1), "xz", (7, 13)),
    (1, (1, 1, 0), "xp", (6, 13)),
    (1, (1, 3, 0), "mx", (7, 13)),
    (1, (0, 1, 1), "pz", (7, 14)),
    (1, (0, 2, 0), "mm", (5, 14)),
    (1, (1, 1, 1), "xzp", (1, 6, 14)),
    (1, (1, 3, 1), "zmx", (2, 6, 14)),
    (1, (0, 0, 1), "z", (15,)),
    (1, (1, 0, 0), "x", (15,)),
    (1, (1, 2, 0), "xpp", (2, 8, 15)),
    (1, (1, 2, 1), "mxzm", (0, 4, 8, 15)),
)
STEPS = 16
AHEAD = 2
PAUSES = 1
SPLIT = 14
TURNS_STEPS = 8
TILE = 128
KEY_PARTS = 4


def plan():
    hops, slots = [], 0
    for array, offset, links, times in ROUTES:
        for at, (link, time) in enumerate(zip(links, times)):
            last = at + 1 == len(links)
            hops.append(
                dict(
                    array=array, offset=offset, at=at, link=link, time=time, done=links[:at],
                    slot=None if last else slots,
                )
            )
            slots += not last
    hops.sort(key=lambda hop: hop["time"])
    where = {(hop["array"], hop["offset"], hop["at"]): i for i, hop in enumerate(hops)}
    for hop in hops:
        hop["after"] = where.get((hop["array"], hop["offset"], hop["at"] - 1))
    return hops, slots


def late_hops(hops):
    return [i for i, hop in enumerate(hops) if hop["time"] >= SPLIT]


def core():
    return lax.axis_index("group") % 2


def device(step):
    z, y, x = lax.axis_index("block"), lax.axis_index("span") // 2, lax.axis_index("span") % 2
    return {"block": (z + step[2]) % 2, "span": ((y + step[1]) % 4) * 2 + (x + step[0]) % 2}


def block_at(dx, dy, dz):
    z, y, x = lax.axis_index("block"), lax.axis_index("span") // 2, lax.axis_index("span") % 2
    return ((z + dz) % 2) * 8 + ((y + dy) % 4) * 2 + (x + dx) % 2


def came_from(offset):
    return block_at(offset[0], 4 - offset[1], offset[2])


def meet():
    barrier = pltpu.get_barrier_semaphore()
    for step in STEP.values():
        pl.semaphore_signal(barrier, inc=1, device_id=device(step), device_id_type=MESH)
    pl.semaphore_wait(barrier, len(STEP))


def kernel(
    hops, angle, gain, keys, values, out_keys, out_values, out_scale, transit,
    raw, table, gain_row, gains, top, send, recv, local,
):
    blocks, rows, size = raw.shape
    half = size // 2
    length = blocks * rows

    me = block_at(0, 0, 0)
    gain_in = pltpu.make_async_copy(gain, gain_row, local.at[0])
    angles_in = pltpu.make_async_copy(angle, table.at[pl.ds(0, half)], local.at[1])
    keys_in = pltpu.make_async_copy(keys.at[me], raw.at[me], local.at[2])
    values_in = pltpu.make_async_copy(values.at[me], out_values.at[me], local.at[3])

    meet()
    copies = [None] * len(hops)
    received = set()

    def arrived(i):
        if i not in received:
            copies[i].wait_recv()
            received.add(i)

    def start(i):
        hop = hops[i]
        if hop["after"] is None:
            source = (keys, values)[hop["array"]].at[block_at(*hop["offset"])]
        else:
            arrived(hop["after"])
            source = transit.at[hops[hop["after"]]["slot"]]
        if hop["slot"] is None:
            gone = [sum(STEP[link][axis] for link in hop["done"]) for axis in range(3)]
            target = (raw, out_values)[hop["array"]].at[block_at(gone[0], 8 - gone[1], gone[2])]
        else:
            target = transit.at[hop["slot"]]
        copies[i] = pltpu.make_async_remote_copy(
            src_ref=source,
            dst_ref=target,
            send_sem=send.at[i],
            recv_sem=recv.at[i],
            device_id=device(STEP[hop["link"]]),
            device_id_type=MESH,
        )
        if hop["time"] < SPLIT:
            copies[i].start()
        else:
            pl.when(core() != PAUSES)(copies[i].start)

    def columns(i):
        return pl.ds(pl.multiple_of(i * TILE, TILE), TILE)

    def turns(begin, end):
        def body(i, _):
            a = table[:half, columns(i)]
            table[:half, columns(i)] = jnp.cos(a)
            table[half:, columns(i)] = jnp.sin(a)
            return 0

        lax.fori_loop(begin, end, body, 0)

    def turn(block):
        def body(i, high):
            at = columns(block * (rows // TILE) + i)
            wide = raw[block, columns(i), :].astype(jnp.float32).T
            mean = jnp.sum(wide * wide, axis=0, keepdims=True) / size
            wide = wide * lax.rsqrt(mean + 1e-06) * gains[...]
            cosine, sine = table[:half, at], table[half:, at]
            first, second = wide[:half], wide[half:]
            one = first * cosine - second * sine
            two = second * cosine + first * sine
            table[:half, at] = one
            table[half:, at] = two
            return jnp.maximum(high, jnp.abs(jnp.concatenate([one, two], axis=0)))

        top[...] = lax.fori_loop(0, rows // TILE, body, top[...])

    def narrow():
        high = jnp.broadcast_to(jnp.max(top[...], axis=1, keepdims=True), (size, TILE))
        top[...] = high
        out_scale[...] = high.T[:1]

        def body(i, _):
            out_keys[:, columns(i)] = (table[:, columns(i)] / top[...]).astype(jnp.bfloat16)
            return 0

        lax.fori_loop(0, length // TILE, body, 0)

    def start_step(time):
        for i, hop in enumerate(hops):
            if hop["time"] == time:
                start(i)

    for copy in (gain_in, angles_in, keys_in, values_in):
        copy.start()
    for time in range(AHEAD):
        start_step(time)
    angles_in.wait()
    gain_in.wait()
    gains[...] = jnp.broadcast_to(gain_row[...], (TILE, size)).T
    top[...] = jnp.zeros_like(top)
    keys_in.wait()
    tiles = length // TILE
    final = [(hop["time"], i) for i, hop in enumerate(hops) if hop["array"] == 0 and hop["slot"] is None]
    for time in range(STEPS):
        start_step(time + AHEAD)
        if time < TURNS_STEPS:
            turns(time * tiles // TURNS_STEPS, (time + 1) * tiles // TURNS_STEPS)
        if time == TURNS_STEPS:
            turn(me)
        for came, i in final:
            if max(came + 1, TURNS_STEPS) == time:
                arrived(i)
                turn(came_from(hops[i]["offset"]))
        if time == max(final)[0] + 1:
            narrow()
    values_in.wait()
    for i, hop in enumerate(hops):
        if hop["time"] < SPLIT:
            arrived(i)
            copies[i].wait_send()

    @pl.when(core() != PAUSES)
    def _():
        for i in late_hops(hops):
            copies[i].wait()


def late(hops, values, transit, _, landed, send, recv):
    @pl.when(core() == PAUSES)
    def _():
        meet()
        copies = []
        for j, i in enumerate(late_hops(hops)):
            hop = hops[i]
            if hop["after"] is None:
                source = values.at[block_at(*hop["offset"])]
            else:
                source = transit.at[hops[hop["after"]]["slot"]]
            copy = pltpu.make_async_remote_copy(
                src_ref=source,
                dst_ref=landed.at[j],
                send_sem=send.at[j],
                recv_sem=recv.at[j],
                device_id=device(STEP[hop["link"]]),
                device_id_type=MESH,
            )
            copy.start()
            copies.append(copy)
        for copy in copies:
            copy.wait()


def store(hops, keys, values, scale, out_keys, out_values, out_scale, done):
    blocks = values.shape[0]
    part = keys.shape[0] // KEY_PARTS
    copies = [pltpu.make_async_copy(scale, out_scale, done.at[0])]
    for i in range(KEY_PARTS):
        at = pl.ds(i * part, part)
        copies.append(pltpu.make_async_copy(keys.at[at], out_keys.at[at], done.at[1 + i]))
    offsets = [hops[i]["offset"] for i in late_hops(hops)]
    offsets += [(0, 0, 0)] + [
        hop["offset"] for hop in hops if hop["array"] == 1 and hop["slot"] is None and hop["time"] < SPLIT
    ]
    moves = []
    for i, offset in enumerate(offsets):
        at = came_from(offset)
        moves.append(
            pltpu.make_async_copy(values.at[at], out_values.at[at], done.at[1 + KEY_PARTS + i])
        )
    assert len(moves) == blocks
    later = len(late_hops(hops))
    for copy in copies + moves[later:]:
        copy.start()

    @pl.when(core() != PAUSES)
    def _():
        for copy in moves[:later]:
            copy.start()
        for copy in moves[:later]:
            copy.wait()

    for copy in copies + moves[later:]:
        copy.wait()


def store_late(hops, landed, stored, out_values, done):
    @pl.when(core() == PAUSES)
    def _():
        copies = []
        for j, i in enumerate(late_hops(hops)):
            target = out_values.at[came_from(hops[i]["offset"])]
            copies.append(pltpu.make_async_copy(landed.at[j], target, done.at[j]))
        for copy in copies:
            copy.start()
        for copy in copies:
            copy.wait()


def body(key_rows, value_rows, turn_angle, key_gain):
    blocks, rows, heads, size = key_rows.shape
    length = blocks * rows
    hops, slots = plan()
    turn_angle, key_gain, key_rows, value_rows = (
        pltpu.with_memory_space_constraint(array, pltpu.HBM)
        for array in (
            turn_angle.T,
            key_gain.reshape(1, size),
            key_rows.reshape(blocks, rows, size),
            value_rows.reshape(blocks, rows, size),
        )
    )
    vmem, hbm = pl.BlockSpec(memory_space=pltpu.VMEM), pl.BlockSpec(memory_space=pl.ANY)
    outputs = (
        ((size, length), jnp.bfloat16),
        ((blocks, rows, size), jnp.bfloat16),
        ((1, size), jnp.float32),
    )
    later = len(late_hops(hops))
    *held, transit = pl.pallas_call(
        functools.partial(kernel, hops),
        name="hand_over",
        out_shape=tuple(pltpu.VMEM(*output) for output in outputs)
        + (pltpu.VMEM((slots, rows, size), jnp.bfloat16),),
        in_specs=[hbm] * 4,
        out_specs=(vmem,) * 4,
        scratch_shapes=[
            pltpu.VMEM((blocks, rows, size), jnp.bfloat16),
            pltpu.VMEM((size, length), jnp.float32),
            pltpu.VMEM((1, size), jnp.float32),
            pltpu.VMEM((size, TILE), jnp.float32),
            pltpu.VMEM((size, TILE), jnp.float32),
            pltpu.SemaphoreType.DMA((len(hops),)),
            pltpu.SemaphoreType.DMA((len(hops),)),
            pltpu.SemaphoreType.DMA((4,)),
        ],
        compiler_params=pltpu.CompilerParams(
            collective_id=0, has_side_effects=True, vmem_limit_bytes=22 << 20
        ),
    )(turn_angle, key_gain, key_rows, value_rows)
    stored_keys, stored_values, key_scale = pl.pallas_call(
        functools.partial(store, hops),
        name="store",
        out_shape=tuple(jax.ShapeDtypeStruct(*output) for output in outputs),
        in_specs=[hbm] * 3,
        out_specs=(hbm,) * 3,
        scratch_shapes=[pltpu.SemaphoreType.DMA((1 + KEY_PARTS + blocks,))],
        compiler_params=pltpu.CompilerParams(vmem_limit_bytes=1 << 20),
    )(*held)
    landed = pl.pallas_call(
        functools.partial(late, hops),
        name="late",
        out_shape=pltpu.VMEM((later, rows, size), jnp.bfloat16),
        in_specs=[hbm] * 3,
        out_specs=vmem,
        scratch_shapes=[pltpu.SemaphoreType.DMA((later,)), pltpu.SemaphoreType.DMA((later,))],
        compiler_params=pltpu.CompilerParams(
            collective_id=1, has_side_effects=True, vmem_limit_bytes=1 << 20
        ),
    )(value_rows, transit, pltpu.with_memory_space_constraint(key_scale, pltpu.HBM))
    stored_values = pl.pallas_call(
        functools.partial(store_late, hops),
        name="store_late",
        out_shape=jax.ShapeDtypeStruct(*outputs[1]),
        in_specs=[hbm] * 2,
        out_specs=hbm,
        scratch_shapes=[pltpu.SemaphoreType.DMA((later,))],
        input_output_aliases={1: 0},
        compiler_params=pltpu.CompilerParams(vmem_limit_bytes=1 << 20),
    )(landed, stored_values)
    return (
        stored_keys.reshape(1, 1, size, length),
        stored_values.reshape(1, length, 1, size),
        key_scale.reshape(1, 1, size),
    )


def solution(mesh):
    return jax.shard_map(
        body,
        mesh=mesh,
        in_specs=(
            P(None, ("block", "span"), "group", None),
            P(None, ("block", "span"), "group", None),
            P(),
            P(),
        ),
        out_specs=(
            P(("block", "span"), "group", None, None),
            P(("block", "span"), None, "group", None),
            P(("block", "span"), "group", None),
        ),
        check_vma=False,
    )
```

```python
import functools

import jax
import jax.numpy as jnp
from jax import lax
from jax.experimental import pallas as pl
from jax.experimental.pallas import tpu as pltpu
from jax.sharding import PartitionSpec as P

MESH = pl.DeviceIdType.MESH
STEP = {"x": (1, 0, 0), "z": (0, 0, 1), "p": (0, 1, 0), "m": (0, 3, 0)}
ROUTES = (
    (0, (0, 2, 0), "mm", (2, 8)),
    (0, (1, 1, 0), "px", (2, 8)),
    (0, (0, 1, 0), "p", (9,)),
    (0, (0, 2, 1), "ppz", (0, 4, 9)),
    (0, (1, 0, 1), "zx", (3, 9)),
    (0, (1, 2, 0), "xmm", (0, 4, 9)),
    (0, (0, 3, 1), "zm", (4, 10)),
    (0, (1, 0, 0), "x", (10,)),
    (0, (1, 2, 1), "zxpp", (0, 3, 6, 10)),
    (0, (1, 3, 1), "mxz", (1, 5, 10)),
    (0, (0, 1, 1), "pz", (3, 11)),
    (0, (0, 3, 0), "m", (11,)),
    (0, (1, 1, 1), "zpx", (1, 5, 11)),
    (0, (0, 0, 1), "z", (12,)),
    (0, (1, 3, 0), "mx", (3, 12)),
    (1, (0, 2, 1), "pzp", (1, 7, 11)),
    (1, (0, 1, 0), "p", (12,)),
    (1, (0, 3, 1), "zm", (5, 12)),
    (1, (0, 3, 0), "m", (13,)),
    (1, (1, 0, 1), "xz", (7, 13)),
    (1, (1, 1, 0), "xp", (6, 13)),
    (1, (1, 3, 0), "mx", (7, 13)),
    (1, (0, 1, 1), "pz", (7, 14)),
    (1, (0, 2, 0), "mm", (5, 14)),
    (1, (1, 1, 1), "xzp", (1, 6, 14)),
    (1, (1, 3, 1), "zmx", (2, 6, 14)),
    (1, (0, 0, 1), "z", (15,)),
    (1, (1, 0, 0), "x", (15,)),
    (1, (1, 2, 0), "xpp", (2, 8, 15)),
    (1, (1, 2, 1), "mxzm", (0, 4, 8, 15)),
)
STEPS = 16
AHEAD = 2
PAUSES = 1
SPLIT, EARLY = 14, 768
TURNS_STEPS = 8
TILE = 128
KEY_PARTS = 4


def plan(rows):
    hops, slots = [], 0
    for array, offset, links, times in ROUTES:
        for at, (link, time) in enumerate(zip(links, times)):
            last = at + 1 == len(links)
            parts = [(0, EARLY), (EARLY, rows - EARLY)] if time == SPLIT else [(0, rows)]
            for begin, count in parts:
                hops.append(
                    dict(
                        array=array, offset=offset, at=at, link=link, time=time, done=links[:at],
                        slot=None if last else slots, begin=begin, count=count,
                        late=time > SPLIT or (time == SPLIT and begin > 0),
                    )
                )
            slots += not last
    hops.sort(key=lambda hop: (hop["time"], hop["begin"]))
    where = {(hop["array"], hop["offset"], hop["at"]): i for i, hop in enumerate(hops)}
    for hop in hops:
        hop["after"] = where.get((hop["array"], hop["offset"], hop["at"] - 1))
    return hops, slots


def late_hops(hops):
    return [i for i, hop in enumerate(hops) if hop["late"]]


def part(hop):
    return pl.ds(hop["begin"], hop["count"])


def core():
    return lax.axis_index("group") % 2


def device(step):
    z, y, x = lax.axis_index("block"), lax.axis_index("span") // 2, lax.axis_index("span") % 2
    return {"block": (z + step[2]) % 2, "span": ((y + step[1]) % 4) * 2 + (x + step[0]) % 2}


def block_at(dx, dy, dz):
    z, y, x = lax.axis_index("block"), lax.axis_index("span") // 2, lax.axis_index("span") % 2
    return ((z + dz) % 2) * 8 + ((y + dy) % 4) * 2 + (x + dx) % 2


def came_from(offset):
    return block_at(offset[0], 4 - offset[1], offset[2])


def meet():
    barrier = pltpu.get_barrier_semaphore()
    for step in STEP.values():
        pl.semaphore_signal(barrier, inc=1, device_id=device(step), device_id_type=MESH)
    pl.semaphore_wait(barrier, len(STEP))


def kernel(
    hops, angle, gain, keys, values, out_keys, out_values, out_scale, transit,
    raw, table, gain_row, gains, top, send, recv, local,
):
    blocks, rows, size = raw.shape
    half = size // 2
    length = blocks * rows

    me = block_at(0, 0, 0)
    gain_in = pltpu.make_async_copy(gain, gain_row, local.at[0])
    angles_in = pltpu.make_async_copy(angle, table.at[pl.ds(0, half)], local.at[1])
    keys_in = pltpu.make_async_copy(keys.at[me], raw.at[me], local.at[2])
    values_in = pltpu.make_async_copy(values.at[me], out_values.at[me], local.at[3])

    meet()
    copies = [None] * len(hops)
    received = set()

    def arrived(i):
        if i not in received:
            copies[i].wait_recv()
            received.add(i)

    def start(i):
        hop = hops[i]
        if hop["after"] is None:
            source = (keys, values)[hop["array"]].at[block_at(*hop["offset"]), part(hop)]
        else:
            arrived(hop["after"])
            source = transit.at[hops[hop["after"]]["slot"], part(hop)]
        if hop["slot"] is None:
            gone = [sum(STEP[link][axis] for link in hop["done"]) for axis in range(3)]
            target = (raw, out_values)[hop["array"]].at[
                block_at(gone[0], 8 - gone[1], gone[2]), part(hop)
            ]
        else:
            target = transit.at[hop["slot"], part(hop)]
        copies[i] = pltpu.make_async_remote_copy(
            src_ref=source,
            dst_ref=target,
            send_sem=send.at[i],
            recv_sem=recv.at[i],
            device_id=device(STEP[hop["link"]]),
            device_id_type=MESH,
        )
        if hop["late"]:
            pl.when(core() != PAUSES)(copies[i].start)
        else:
            copies[i].start()

    def columns(i):
        return pl.ds(pl.multiple_of(i * TILE, TILE), TILE)

    def turns(begin, end):
        def body(i, _):
            a = table[:half, columns(i)]
            table[:half, columns(i)] = jnp.cos(a)
            table[half:, columns(i)] = jnp.sin(a)
            return 0

        lax.fori_loop(begin, end, body, 0)

    def turn(block):
        def body(i, high):
            at = columns(block * (rows // TILE) + i)
            wide = raw[block, columns(i), :].astype(jnp.float32).T
            mean = jnp.sum(wide * wide, axis=0, keepdims=True) / size
            wide = wide * lax.rsqrt(mean + 1e-06) * gains[...]
            cosine, sine = table[:half, at], table[half:, at]
            first, second = wide[:half], wide[half:]
            one = first * cosine - second * sine
            two = second * cosine + first * sine
            table[:half, at] = one
            table[half:, at] = two
            return jnp.maximum(high, jnp.abs(jnp.concatenate([one, two], axis=0)))

        top[...] = lax.fori_loop(0, rows // TILE, body, top[...])

    def narrow():
        high = jnp.broadcast_to(jnp.max(top[...], axis=1, keepdims=True), (size, TILE))
        top[...] = high
        out_scale[...] = high.T[:1]

        def body(i, _):
            out_keys[:, columns(i)] = (table[:, columns(i)] / top[...]).astype(jnp.bfloat16)
            return 0

        lax.fori_loop(0, length // TILE, body, 0)

    def start_step(time):
        for i, hop in enumerate(hops):
            if hop["time"] == time:
                start(i)

    for copy in (gain_in, angles_in, keys_in, values_in):
        copy.start()
    pl.when(core() != PAUSES)(angles_in.wait)
    for time in range(AHEAD):
        start_step(time)
    pl.when(core() == PAUSES)(angles_in.wait)
    gain_in.wait()
    gains[...] = jnp.broadcast_to(gain_row[...], (TILE, size)).T
    top[...] = jnp.zeros_like(top)
    keys_in.wait()
    tiles = length // TILE
    final = [(hop["time"], i) for i, hop in enumerate(hops) if hop["array"] == 0 and hop["slot"] is None]
    for time in range(STEPS):
        start_step(time + AHEAD)
        if time < TURNS_STEPS:
            turns(time * tiles // TURNS_STEPS, (time + 1) * tiles // TURNS_STEPS)
        if time == TURNS_STEPS:
            turn(me)
        for came, i in final:
            if max(came + 1, TURNS_STEPS) == time:
                arrived(i)
                turn(came_from(hops[i]["offset"]))
        if time == max(final)[0] + 1:
            narrow()
    values_in.wait()
    for i, hop in enumerate(hops):
        if not hop["late"]:
            arrived(i)
            copies[i].wait_send()

    @pl.when(core() != PAUSES)
    def _():
        for i in late_hops(hops):
            copies[i].wait()


def late(hops, values, transit, _, landed, send, recv):
    @pl.when(core() == PAUSES)
    def _():
        meet()
        copies = []
        for j, i in enumerate(late_hops(hops)):
            hop = hops[i]
            if hop["after"] is None:
                source = values.at[block_at(*hop["offset"]), part(hop)]
            else:
                source = transit.at[hops[hop["after"]]["slot"], part(hop)]
            copy = pltpu.make_async_remote_copy(
                src_ref=source,
                dst_ref=landed.at[j, part(hop)],
                send_sem=send.at[j],
                recv_sem=recv.at[j],
                device_id=device(STEP[hop["link"]]),
                device_id_type=MESH,
            )
            copy.start()
            copies.append(copy)
        for copy in copies:
            copy.wait()


def store(hops, keys, values, scale, out_keys, out_values, out_scale, done):
    size = keys.shape[0] // KEY_PARTS
    copies = [pltpu.make_async_copy(scale, out_scale, done.at[0])]
    for i in range(KEY_PARTS):
        at = pl.ds(i * size, size)
        copies.append(pltpu.make_async_copy(keys.at[at], out_keys.at[at], done.at[1 + i]))
    own = dict(offset=(0, 0, 0), begin=0, count=values.shape[1])
    final = [hop for hop in hops if hop["array"] == 1 and hop["slot"] is None and not hop["late"]]
    moves = []
    for i, hop in enumerate([hops[i] for i in late_hops(hops)] + [own] + final):
        at = came_from(hop["offset"])
        moves.append(
            pltpu.make_async_copy(
                values.at[at, part(hop)], out_values.at[at, part(hop)], done.at[1 + KEY_PARTS + i]
            )
        )
    later = len(late_hops(hops))
    for copy in copies + moves[later:]:
        copy.start()

    @pl.when(core() != PAUSES)
    def _():
        for copy in moves[:later]:
            copy.start()
        for copy in moves[:later]:
            copy.wait()

    for copy in copies + moves[later:]:
        copy.wait()


def store_late(hops, landed, stored, out_values, done):
    @pl.when(core() == PAUSES)
    def _():
        copies = []
        for j, i in enumerate(late_hops(hops)):
            rows = part(hops[i])
            target = out_values.at[came_from(hops[i]["offset"]), rows]
            copies.append(pltpu.make_async_copy(landed.at[j, rows], target, done.at[j]))
        for copy in copies:
            copy.start()
        for copy in copies:
            copy.wait()


def body(key_rows, value_rows, turn_angle, key_gain):
    blocks, rows, heads, size = key_rows.shape
    length = blocks * rows
    hops, slots = plan(rows)
    turn_angle, key_gain, key_rows, value_rows = (
        pltpu.with_memory_space_constraint(array, pltpu.HBM)
        for array in (
            turn_angle.T,
            key_gain.reshape(1, size),
            key_rows.reshape(blocks, rows, size),
            value_rows.reshape(blocks, rows, size),
        )
    )
    vmem, hbm = pl.BlockSpec(memory_space=pltpu.VMEM), pl.BlockSpec(memory_space=pl.ANY)
    outputs = (
        ((size, length), jnp.bfloat16),
        ((blocks, rows, size), jnp.bfloat16),
        ((1, size), jnp.float32),
    )
    later = len(late_hops(hops))
    *held, transit = pl.pallas_call(
        functools.partial(kernel, hops),
        name="hand_over",
        out_shape=tuple(pltpu.VMEM(*output) for output in outputs)
        + (pltpu.VMEM((slots, rows, size), jnp.bfloat16),),
        in_specs=[hbm] * 4,
        out_specs=(vmem,) * 4,
        scratch_shapes=[
            pltpu.VMEM((blocks, rows, size), jnp.bfloat16),
            pltpu.VMEM((size, length), jnp.float32),
            pltpu.VMEM((1, size), jnp.float32),
            pltpu.VMEM((size, TILE), jnp.float32),
            pltpu.VMEM((size, TILE), jnp.float32),
            pltpu.SemaphoreType.DMA((len(hops),)),
            pltpu.SemaphoreType.DMA((len(hops),)),
            pltpu.SemaphoreType.DMA((4,)),
        ],
        compiler_params=pltpu.CompilerParams(
            collective_id=0, has_side_effects=True, vmem_limit_bytes=22 << 20
        ),
    )(turn_angle, key_gain, key_rows, value_rows)
    stored_keys, stored_values, key_scale = pl.pallas_call(
        functools.partial(store, hops),
        name="store",
        out_shape=tuple(jax.ShapeDtypeStruct(*output) for output in outputs),
        in_specs=[hbm] * 3,
        out_specs=(hbm,) * 3,
        scratch_shapes=[pltpu.SemaphoreType.DMA((1 + KEY_PARTS + blocks + len(hops),))],
        compiler_params=pltpu.CompilerParams(vmem_limit_bytes=1 << 20),
    )(*held)
    landed = pl.pallas_call(
        functools.partial(late, hops),
        name="late",
        out_shape=pltpu.VMEM((later, rows, size), jnp.bfloat16),
        in_specs=[hbm] * 3,
        out_specs=vmem,
        scratch_shapes=[pltpu.SemaphoreType.DMA((later,)), pltpu.SemaphoreType.DMA((later,))],
        compiler_params=pltpu.CompilerParams(
            collective_id=1, has_side_effects=True, vmem_limit_bytes=1 << 20
        ),
    )(value_rows, transit, pltpu.with_memory_space_constraint(key_scale, pltpu.HBM))
    stored_values = pl.pallas_call(
        functools.partial(store_late, hops),
        name="store_late",
        out_shape=jax.ShapeDtypeStruct(*outputs[1]),
        in_specs=[hbm] * 2,
        out_specs=hbm,
        scratch_shapes=[pltpu.SemaphoreType.DMA((later,))],
        input_output_aliases={1: 0},
        compiler_params=pltpu.CompilerParams(vmem_limit_bytes=1 << 20),
    )(landed, stored_values)
    return (
        stored_keys.reshape(1, 1, size, length),
        stored_values.reshape(1, length, 1, size),
        key_scale.reshape(1, 1, size),
    )


def solution(mesh):
    return jax.shard_map(
        body,
        mesh=mesh,
        in_specs=(
            P(None, ("block", "span"), "group", None),
            P(None, ("block", "span"), "group", None),
            P(),
            P(),
        ),
        out_specs=(
            P(("block", "span"), "group", None, None),
            P(("block", "span"), None, "group", None),
            P(("block", "span"), "group", None),
        ),
        check_vma=False,
    )
```

```python
import functools

import jax
import jax.numpy as jnp
from jax import lax
from jax.experimental import pallas as pl
from jax.experimental.pallas import tpu as pltpu
from jax.sharding import PartitionSpec as P

MESH = pl.DeviceIdType.MESH
STEP = {"x": (1, 0, 0), "z": (0, 0, 1), "p": (0, 1, 0), "m": (0, 3, 0)}
ROUTES = (
    (0, (0, 2, 0), "mm", (2, 8)),
    (0, (1, 1, 0), "px", (2, 8)),
    (0, (0, 1, 0), "p", (9,)),
    (0, (0, 2, 1), "ppz", (0, 4, 9)),
    (0, (1, 0, 1), "zx", (3, 9)),
    (0, (1, 2, 0), "xmm", (0, 4, 9)),
    (0, (0, 3, 1), "zm", (4, 10)),
    (0, (1, 0, 0), "x", (10,)),
    (0, (1, 2, 1), "zxpp", (0, 3, 6, 10)),
    (0, (1, 3, 1), "mxz", (1, 5, 10)),
    (0, (0, 1, 1), "pz", (3, 11)),
    (0, (0, 3, 0), "m", (11,)),
    (0, (1, 1, 1), "zpx", (1, 5, 11)),
    (0, (0, 0, 1), "z", (12,)),
    (0, (1, 3, 0), "mx", (3, 12)),
    (1, (0, 2, 1), "pzp", (1, 7, 11)),
    (1, (0, 1, 0), "p", (12,)),
    (1, (0, 3, 1), "zm", (5, 12)),
    (1, (0, 3, 0), "m", (13,)),
    (1, (1, 0, 1), "xz", (7, 13)),
    (1, (1, 1, 0), "xp", (6, 13)),
    (1, (1, 3, 0), "mx", (7, 13)),
    (1, (0, 1, 1), "pz", (7, 14)),
    (1, (0, 2, 0), "mm", (5, 14)),
    (1, (1, 1, 1), "xzp", (1, 6, 14)),
    (1, (1, 3, 1), "zmx", (2, 6, 14)),
    (1, (0, 0, 1), "z", (15,)),
    (1, (1, 0, 0), "x", (15,)),
    (1, (1, 2, 0), "xpp", (2, 8, 15)),
    (1, (1, 2, 1), "mxzm", (0, 4, 8, 15)),
)
STEPS = 16
AHEAD = 2
PAUSES = 1
SPLIT, EARLY = 14, 768
TURNS_STEPS = 8
TILE = 128
KEY_PARTS = 4


def plan(rows):
    hops, slots = [], 0
    for array, offset, links, times in ROUTES:
        for at, (link, time) in enumerate(zip(links, times)):
            last = at + 1 == len(links)
            parts = [(0, EARLY), (EARLY, rows - EARLY)] if time == SPLIT else [(0, rows)]
            for begin, count in parts:
                hops.append(
                    dict(
                        array=array, offset=offset, at=at, link=link, time=time, done=links[:at],
                        slot=None if last else slots, begin=begin, count=count,
                        late=time > SPLIT or (time == SPLIT and begin > 0),
                    )
                )
            slots += not last
    hops.sort(key=lambda hop: (hop["time"], hop["begin"]))
    where = {(hop["array"], hop["offset"], hop["at"]): i for i, hop in enumerate(hops)}
    for hop in hops:
        hop["after"] = where.get((hop["array"], hop["offset"], hop["at"] - 1))
    return hops, slots


def late_hops(hops):
    return [i for i, hop in enumerate(hops) if hop["late"]]


def early_values(hops):
    return [hop for hop in hops if hop["array"] == 1 and hop["slot"] is None and not hop["late"]]


def part(hop):
    return pl.ds(hop["begin"], hop["count"])


def core():
    return lax.axis_index("group") % 2


def device(step):
    z, y, x = lax.axis_index("block"), lax.axis_index("span") // 2, lax.axis_index("span") % 2
    return {"block": (z + step[2]) % 2, "span": ((y + step[1]) % 4) * 2 + (x + step[0]) % 2}


def block_at(dx, dy, dz):
    z, y, x = lax.axis_index("block"), lax.axis_index("span") // 2, lax.axis_index("span") % 2
    return ((z + dz) % 2) * 8 + ((y + dy) % 4) * 2 + (x + dx) % 2


def came_from(offset):
    return block_at(offset[0], 4 - offset[1], offset[2])


def meet():
    barrier = pltpu.get_barrier_semaphore()
    for step in STEP.values():
        pl.semaphore_signal(barrier, inc=1, device_id=device(step), device_id_type=MESH)
    pl.semaphore_wait(barrier, len(STEP))


def kernel(
    hops, angle, gain, keys, values, out_keys, out_values, out_scale, transit,
    raw, table, gain_row, gains, top, send, recv, local,
):
    blocks, rows, size = raw.shape
    half = size // 2
    length = blocks * rows

    me = block_at(0, 0, 0)
    gain_in = pltpu.make_async_copy(gain, gain_row, local.at[0])
    angles_in = pltpu.make_async_copy(angle, table.at[pl.ds(0, half)], local.at[1])
    keys_in = pltpu.make_async_copy(keys.at[me], raw.at[me], local.at[2])
    values_in = pltpu.make_async_copy(values.at[me], out_values.at[me], local.at[3])

    meet()
    copies = [None] * len(hops)
    received = set()

    def arrived(i):
        if i not in received:
            copies[i].wait_recv()
            received.add(i)

    def start(i):
        hop = hops[i]
        if hop["after"] is None:
            source = (keys, values)[hop["array"]].at[block_at(*hop["offset"]), part(hop)]
        else:
            arrived(hop["after"])
            source = transit.at[hops[hop["after"]]["slot"], part(hop)]
        if hop["slot"] is None:
            gone = [sum(STEP[link][axis] for link in hop["done"]) for axis in range(3)]
            target = (raw, out_values)[hop["array"]].at[
                block_at(gone[0], 8 - gone[1], gone[2]), part(hop)
            ]
        else:
            target = transit.at[hop["slot"], part(hop)]
        copies[i] = pltpu.make_async_remote_copy(
            src_ref=source,
            dst_ref=target,
            send_sem=send.at[i],
            recv_sem=recv.at[i],
            device_id=device(STEP[hop["link"]]),
            device_id_type=MESH,
        )
        if hop["late"]:
            pl.when(core() != PAUSES)(copies[i].start)
        else:
            copies[i].start()

    def columns(i):
        return pl.ds(pl.multiple_of(i * TILE, TILE), TILE)

    def turns(begin, end):
        def body(i, _):
            a = table[:half, columns(i)]
            table[:half, columns(i)] = jnp.cos(a)
            table[half:, columns(i)] = jnp.sin(a)
            return 0

        lax.fori_loop(begin, end, body, 0)

    def turn(block):
        def body(i, high):
            at = columns(block * (rows // TILE) + i)
            wide = raw[block, columns(i), :].astype(jnp.float32).T
            mean = jnp.sum(wide * wide, axis=0, keepdims=True) / size
            wide = wide * lax.rsqrt(mean + 1e-06) * gains[...]
            cosine, sine = table[:half, at], table[half:, at]
            first, second = wide[:half], wide[half:]
            one = first * cosine - second * sine
            two = second * cosine + first * sine
            table[:half, at] = one
            table[half:, at] = two
            return jnp.maximum(high, jnp.abs(jnp.concatenate([one, two], axis=0)))

        top[...] = lax.fori_loop(0, rows // TILE, body, top[...])

    def narrow():
        high = jnp.broadcast_to(jnp.max(top[...], axis=1, keepdims=True), (size, TILE))
        top[...] = high
        out_scale[...] = high.T[:1]

        def body(i, _):
            out_keys[:, columns(i)] = (table[:, columns(i)] / top[...]).astype(jnp.bfloat16)
            return 0

        lax.fori_loop(0, length // TILE, body, 0)

    def start_step(time):
        for i, hop in enumerate(hops):
            if hop["time"] == time:
                start(i)

    for copy in (gain_in, angles_in, keys_in, values_in):
        copy.start()
    pl.when(core() != PAUSES)(angles_in.wait)
    for time in range(AHEAD):
        start_step(time)
    pl.when(core() == PAUSES)(angles_in.wait)
    gain_in.wait()
    gains[...] = jnp.broadcast_to(gain_row[...], (TILE, size)).T
    top[...] = jnp.zeros_like(top)
    keys_in.wait()
    tiles = length // TILE
    final = [(hop["time"], i) for i, hop in enumerate(hops) if hop["array"] == 0 and hop["slot"] is None]
    for time in range(STEPS):
        start_step(time + AHEAD)
        if time < TURNS_STEPS:
            turns(time * tiles // TURNS_STEPS, (time + 1) * tiles // TURNS_STEPS)
        if time == TURNS_STEPS:
            turn(me)
        for came, i in final:
            if max(came + 1, TURNS_STEPS) == time:
                arrived(i)
                turn(came_from(hops[i]["offset"]))
        if time == max(final)[0] + 1:
            narrow()
    values_in.wait()
    for i, hop in enumerate(hops):
        if not hop["late"]:
            arrived(i)
            copies[i].wait_send()

    @pl.when(core() != PAUSES)
    def _():
        for i in late_hops(hops):
            copies[i].wait()


def late(hops, values, transit, _, landed, send, recv):
    @pl.when(core() == PAUSES)
    def _():
        meet()
        copies = []
        for j, i in enumerate(late_hops(hops)):
            hop = hops[i]
            if hop["after"] is None:
                source = values.at[block_at(*hop["offset"]), part(hop)]
            else:
                source = transit.at[hops[hop["after"]]["slot"], part(hop)]
            copy = pltpu.make_async_remote_copy(
                src_ref=source,
                dst_ref=landed.at[j, part(hop)],
                send_sem=send.at[j],
                recv_sem=recv.at[j],
                device_id=device(STEP[hop["link"]]),
                device_id_type=MESH,
            )
            copy.start()
            copies.append(copy)
        for copy in copies:
            copy.wait()


def store(hops, keys, values, scale, out_keys, out_values, out_scale, done):
    size = keys.shape[0] // KEY_PARTS
    copies = [pltpu.make_async_copy(scale, out_scale, done.at[0])]
    for i in range(KEY_PARTS):
        at = pl.ds(i * size, size)
        copies.append(pltpu.make_async_copy(keys.at[at], out_keys.at[at], done.at[1 + i]))
    own = dict(offset=(0, 0, 0), begin=0, count=values.shape[1])
    moves = []
    for i, hop in enumerate([own] + early_values(hops)):
        at = came_from(hop["offset"])
        moves.append(
            pltpu.make_async_copy(
                values.at[at, part(hop)], out_values.at[at, part(hop)], done.at[1 + KEY_PARTS + i]
            )
        )
    step = values.shape[0] // KEY_PARTS
    whole = []
    for i in range(KEY_PARTS):
        at = pl.ds(i * step, step)
        whole.append(
            pltpu.make_async_copy(values.at[at], out_values.at[at], done.at[1 + KEY_PARTS + i])
        )
    for copy in copies:
        copy.start()
    for mine, group in ((core() == PAUSES, moves), (core() != PAUSES, whole)):

        @pl.when(mine)
        def _(group=group):
            for copy in group:
                copy.start()
            for copy in group:
                copy.wait()

    for copy in copies:
        copy.wait()


def store_late(hops, landed, stored, out_values, done):
    @pl.when(core() == PAUSES)
    def _():
        copies = []
        for j, i in enumerate(late_hops(hops)):
            rows = part(hops[i])
            target = out_values.at[came_from(hops[i]["offset"]), rows]
            copies.append(pltpu.make_async_copy(landed.at[j, rows], target, done.at[j]))
        for copy in copies:
            copy.start()
        for copy in copies:
            copy.wait()


def body(key_rows, value_rows, turn_angle, key_gain):
    blocks, rows, heads, size = key_rows.shape
    length = blocks * rows
    hops, slots = plan(rows)
    turn_angle, key_gain, key_rows, value_rows = (
        pltpu.with_memory_space_constraint(array, pltpu.HBM)
        for array in (
            turn_angle.T,
            key_gain.reshape(1, size),
            key_rows.reshape(blocks, rows, size),
            value_rows.reshape(blocks, rows, size),
        )
    )
    vmem, hbm = pl.BlockSpec(memory_space=pltpu.VMEM), pl.BlockSpec(memory_space=pl.ANY)
    outputs = (
        ((size, length), jnp.bfloat16),
        ((blocks, rows, size), jnp.bfloat16),
        ((1, size), jnp.float32),
    )
    later = len(late_hops(hops))
    *held, transit = pl.pallas_call(
        functools.partial(kernel, hops),
        name="hand_over",
        out_shape=tuple(pltpu.VMEM(*output) for output in outputs)
        + (pltpu.VMEM((slots, rows, size), jnp.bfloat16),),
        in_specs=[hbm] * 4,
        out_specs=(vmem,) * 4,
        scratch_shapes=[
            pltpu.VMEM((blocks, rows, size), jnp.bfloat16),
            pltpu.VMEM((size, length), jnp.float32),
            pltpu.VMEM((1, size), jnp.float32),
            pltpu.VMEM((size, TILE), jnp.float32),
            pltpu.VMEM((size, TILE), jnp.float32),
            pltpu.SemaphoreType.DMA((len(hops),)),
            pltpu.SemaphoreType.DMA((len(hops),)),
            pltpu.SemaphoreType.DMA((4,)),
        ],
        compiler_params=pltpu.CompilerParams(
            collective_id=0, has_side_effects=True, vmem_limit_bytes=22 << 20
        ),
    )(turn_angle, key_gain, key_rows, value_rows)
    stored_keys, stored_values, key_scale = pl.pallas_call(
        functools.partial(store, hops),
        name="store",
        out_shape=tuple(jax.ShapeDtypeStruct(*output) for output in outputs),
        in_specs=[hbm] * 3,
        out_specs=(hbm,) * 3,
        scratch_shapes=[pltpu.SemaphoreType.DMA((2 + KEY_PARTS + len(early_values(hops)),))],
        compiler_params=pltpu.CompilerParams(vmem_limit_bytes=1 << 20),
    )(*held)
    landed = pl.pallas_call(
        functools.partial(late, hops),
        name="late",
        out_shape=pltpu.VMEM((later, rows, size), jnp.bfloat16),
        in_specs=[hbm] * 3,
        out_specs=vmem,
        scratch_shapes=[pltpu.SemaphoreType.DMA((later,)), pltpu.SemaphoreType.DMA((later,))],
        compiler_params=pltpu.CompilerParams(
            collective_id=1, has_side_effects=True, vmem_limit_bytes=1 << 20
        ),
    )(value_rows, transit, pltpu.with_memory_space_constraint(key_scale, pltpu.HBM))
    stored_values = pl.pallas_call(
        functools.partial(store_late, hops),
        name="store_late",
        out_shape=jax.ShapeDtypeStruct(*outputs[1]),
        in_specs=[hbm] * 2,
        out_specs=hbm,
        scratch_shapes=[pltpu.SemaphoreType.DMA((later,))],
        input_output_aliases={1: 0},
        compiler_params=pltpu.CompilerParams(vmem_limit_bytes=1 << 20),
    )(landed, stored_values)
    return (
        stored_keys.reshape(1, 1, size, length),
        stored_values.reshape(1, length, 1, size),
        key_scale.reshape(1, 1, size),
    )


def solution(mesh):
    return jax.shard_map(
        body,
        mesh=mesh,
        in_specs=(
            P(None, ("block", "span"), "group", None),
            P(None, ("block", "span"), "group", None),
            P(),
            P(),
        ),
        out_specs=(
            P(("block", "span"), "group", None, None),
            P(("block", "span"), None, "group", None),
            P(("block", "span"), "group", None),
        ),
        check_vma=False,
    )
```
